32 devices in a mesh: section: 4 (over x, core), tp: 8 (over z, y).
Axes of the slice: x: 2, y: 2, z: 4, core: 2. Of those that a mesh axis runs over, the one named last changes fastest.
Arguments:
- pending_activation: bfloat16 [4, 128, 4096], P('section'), may hold values from -6 to 6
- admissible_microbatches: bfloat16 [4, 128, 4096], P(None, None, 'tp'), may hold values from -6 to 6
- arrival_plan: int32 [4], replicated, may hold values from 0 to 3, each once
- vanished_hop: int32 [1], replicated, may hold values from 1 to 3
- query_key_value_matrices: bfloat16 [4, 4096, 3, 2048], P('section', None, None, 'tp')
- mixing_projection_matrices: bfloat16 [4, 2048, 4096], P('section', 'tp'), may hold values from -0.125 to 0.125
- normalizer_factors: bfloat16 [4, 4096], P('section'), may hold values from 0.25 to 1.75
Outputs:
- activation_later: bfloat16 [4, 128, 4096], P('section')
- standby_input: bfloat16 [4, 128, 4096], P('section', None, 'tp')
The draws below stay inside these ranges and needn't reach their ends.
Inputs may be any that keep to these rules, and one draw needn't show every extreme that they name: `vanished_hop`: the preempted section is not the first. `arrival_plan`: each micro-batch index once.
All inputs are finite; a program needn't handle non-finite values.
Results may differ from the reference program's by a relative error of at most 0.013.
Values may be sent and summed in bfloat16 or wider, within the bound.
A program may use at most 64 MiB of HBM per device.

```python
import jax
import jax.numpy as jnp
from jax import lax

HIDDEN_SIZE = 4096
HEADS = 16
HD = 128
STRING_LENGTH = 128
TICKS = 3
POOL = 4
LAYER_HOPS = 4


def draw_query_key_value_matrices(key, part):
    base = jax.random.normal(key, (LAYER_HOPS, HIDDEN_SIZE, 3, HEADS * HD), jnp.float32) * HIDDEN_SIZE ** (-0.5)
    return base.astype(jnp.bfloat16)


def level_of(stream_key, dims, pieces, low, high):
    loudness = 1.0
    for position, shards_of in pieces:
        draws = jax.random.uniform(jax.random.fold_in(jax.random.fold_in(stream_key, 6), position), (shards_of,), jnp.float32, low / len(pieces), high / len(pieces))
        loudness = loudness * jnp.repeat(jnp.exp(draws), dims[position] // shards_of).reshape((-1,) + (1,) * (len(dims) - 1 - position))
    return loudness


def bell_draw(rng, dims, width, limit, cuts=(), held_as=jnp.bfloat16):
    array = jax.random.normal(rng, dims, jnp.float32) * width
    if len(cuts) > 0:
        array = level_of(rng, dims, cuts, -0.22, 0.18) * array
    return jnp.clip(array, min=-limit, max=limit).astype(held_as)


def setup_inputs(seed: int = 0) -> dict:
    arg_keys = jax.random.split(jax.random.key(seed), 8)
    pending_activation = bell_draw(arg_keys[0], (LAYER_HOPS, STRING_LENGTH, HIDDEN_SIZE), 1.0, 6.0, ((0, 4),))
    admissible_microbatches = bell_draw(arg_keys[1], (POOL, STRING_LENGTH, HIDDEN_SIZE), 1.0, 6.0, ((2, 8),))
    arrival_plan = jax.random.permutation(arg_keys[2], POOL).astype(jnp.int32)
    vanished_hop = jax.random.randint(arg_keys[3], (1,), 1, LAYER_HOPS).astype(jnp.int32)
    query_key_value_matrices = draw_query_key_value_matrices(jax.random.fold_in(arg_keys[7], 71), 0)
    mixing_projection_matrices = bell_draw(arg_keys[5], (LAYER_HOPS, HEADS * HD, HIDDEN_SIZE), (HEADS * HD) ** -0.5, 0.125, ((0, 4), (1, 8)))
    normalizer_factors = jnp.clip(1.0 + 0.15 * jax.random.normal(arg_keys[6], (LAYER_HOPS, HIDDEN_SIZE), jnp.float32), 0.25, 1.75).astype(jnp.bfloat16)
    return dict(pending_activation=pending_activation, admissible_microbatches=admissible_microbatches, arrival_plan=arrival_plan, vanished_hop=vanished_hop, query_key_value_matrices=query_key_value_matrices, mixing_projection_matrices=mixing_projection_matrices, normalizer_factors=normalizer_factors)


NORM_EPS = 1e-05

def layer_norm(x_rows, scale_row):
    widened = x_rows.astype(jnp.float32)
    row_mean = lax.optimization_barrier(jnp.mean(widened, axis=-1, keepdims=True))
    centered = widened - row_mean
    row_var = lax.optimization_barrier(jnp.mean(centered * centered, axis=-1, keepdims=True))
    return (centered * lax.rsqrt(row_var + NORM_EPS) * scale_row.astype(jnp.float32)).astype(jnp.bfloat16)

def attend(normed, w_in, w_out):
    row_count = normed.shape[0]
    col_count = w_in.shape[2]
    head_count = col_count // HD
    projected = jnp.dot(normed, w_in.reshape(w_in.shape[0], 3 * col_count), preferred_element_type=jnp.float32)
    projected = projected.astype(jnp.bfloat16).reshape(row_count, 3, head_count, HD)
    queries = projected[:, 0].astype(jnp.float32)
    key_rows = projected[:, 1].astype(jnp.float32)
    values = projected[:, 2].astype(jnp.float32)
    scores = jnp.einsum('qhd,khd->hqk', queries, key_rows) * HD ** (-0.5)
    causal = jnp.arange(row_count)[:, None] >= jnp.arange(row_count)[None, :]
    scores = jnp.where(causal[None], scores, -jnp.inf)
    row_max = lax.optimization_barrier(jnp.max(scores, axis=-1, keepdims=True))
    weights = jnp.exp(scores - row_max)
    probs = (weights / lax.optimization_barrier(jnp.sum(weights, axis=-1, keepdims=True))).astype(jnp.bfloat16)
    context = jnp.einsum('hqk,khd->qhd', probs.astype(jnp.float32), values)
    context = context.astype(jnp.bfloat16).reshape(row_count, col_count)
    return jnp.dot(context, w_out, preferred_element_type=jnp.float32)

def section_layer(x_rows, w_in, w_out, scale_row):
    branch = attend(layer_norm(x_rows, scale_row), w_in, w_out)
    return (x_rows.astype(jnp.float32) + branch).astype(jnp.bfloat16)

def reference(pending_activation, admissible_microbatches, arrival_plan, vanished_hop, query_key_value_matrices, mixing_projection_matrices, normalizer_factors):
    lost_at = vanished_hop[0]
    section_ids = jnp.arange(LAYER_HOPS)[:, None, None]
    activation_later = pending_activation
    spares = None
    for tick_index in range(TICKS):
        outputs = lax.map(lambda operands: section_layer(*operands), (activation_later, query_key_value_matrices, mixing_projection_matrices, normalizer_factors))
        if tick_index == TICKS - 1:
            spares = lax.map(lambda operands: section_layer(*operands), (outputs, jnp.roll(query_key_value_matrices, -1, axis=0), jnp.roll(mixing_projection_matrices, -1, axis=0), jnp.roll(normalizer_factors, -1, axis=0)))
            redone = lax.dynamic_index_in_dim(spares, lost_at - 1, 0, keepdims=False)
        else:
            earlier = lax.dynamic_index_in_dim(outputs, lost_at - 1, 0, keepdims=False)
            redone = section_layer(earlier, lax.dynamic_index_in_dim(query_key_value_matrices, lost_at, 0, keepdims=False), lax.dynamic_index_in_dim(mixing_projection_matrices, lost_at, 0, keepdims=False), lax.dynamic_index_in_dim(normalizer_factors, lost_at, 0, keepdims=False))
        outputs = lax.dynamic_update_index_in_dim(outputs, redone, lost_at - 1, 0)
        entering = lax.dynamic_index_in_dim(admissible_microbatches, arrival_plan[tick_index], 0, keepdims=True)
        shifted = jnp.concatenate([entering, outputs[:-1]], axis=0)
        activation_later = jnp.where(section_ids == lost_at, jnp.zeros_like(shifted), jnp.where(section_ids == lost_at + 1, redone[None], shifted))
    standby_input = jnp.roll(spares, 2, axis=0)
    return (activation_later, standby_input)
```

```python
import functools

import jax
import jax.numpy as jnp
from jax import lax
from jax.experimental import pallas as pl
from jax.experimental.pallas import tpu as pltpu
from jax.sharding import PartitionSpec as P

HD = 128
TICKS = 3
NORM_EPS = 1e-05
MESH = pl.DeviceIdType.MESH


def relay_kernel(
    sections, nz, ny,
    lost_ref, plan_ref, pend_ref, pool_ref, win_ref, wout_ref, gain_ref,
    later_ref, standby_ref,
    x_buf, y_buf, acc, qkv, ctx, part, own_part, ry_buf, zs_buf, rz_buf, fwd_buf, last_buf, spare_in,
    ag_zs, ag_zr, ag_ys, ag_yr, rs_zs, rs_zr, rs_ys, rs_yr, sh_s, sh_r,
):
    steps = TICKS + 2
    s = lax.axis_index("section")
    me = lax.axis_index("tp")
    z, y = me // ny, me % ny
    nxt, prv = (s + 1) % sections, (s + sections - 1) % sections
    lost = lost_ref[0]
    devices = nz * ny
    rows, width = x_buf.shape[2], x_buf.shape[3]
    cols = wout_ref.shape[0]
    heads = cols // HD

    def tp_at(dz, dy):
        return ((z + dz + nz) % nz) * ny + (y + dy + ny) % ny

    barrier = pltpu.get_barrier_semaphore()
    for dz in range(1, nz):
        pl.semaphore_signal(barrier, inc=1, device_id={"section": s, "tp": tp_at(dz, 0)}, device_id_type=MESH)
    for dy in range(1, ny):
        pl.semaphore_signal(barrier, inc=1, device_id={"section": s, "tp": tp_at(0, dy)}, device_id_type=MESH)
    pl.semaphore_signal(barrier, inc=1, device_id={"section": nxt, "tp": me}, device_id_type=MESH)
    pl.semaphore_signal(barrier, inc=1, device_id={"section": prv, "tp": me}, device_id_type=MESH)
    pl.semaphore_wait(barrier, nz + ny)

    def copy_to(src, dst, send, recv, section, tp):
        return pltpu.make_async_remote_copy(
            src_ref=src, dst_ref=dst, send_sem=send, recv_sem=recv,
            device_id={"section": section, "tp": tp}, device_id_type=MESH,
        )

    def block_copy(n, slot, send, recv, tp):
        return copy_to(x_buf.at[n, slot], x_buf.at[n, slot], send, recv, s, tp)

    def all_gather(n):
        sends = []
        for dz in range(1, nz):
            sends.append(block_copy(n, me, ag_zs.at[dz], ag_zr.at[n, dz], tp_at(dz, 0)))
            sends[-1].start()
        for dz in range(nz):
            slot = tp_at(-dz, 0)
            if dz:
                block_copy(n, slot, ag_zs.at[dz], ag_zr.at[n, dz], tp_at(dz, 0)).wait_recv()
            for dy in range(1, ny):
                sends.append(block_copy(n, slot, ag_ys.at[dz, dy], ag_yr.at[n, dz, dy], tp_at(0, dy)))
                sends[-1].start()
        for dz in range(nz):
            for dy in range(1, ny):
                slot = tp_at(-dz, -dy)
                block_copy(n, slot, ag_ys.at[dz, dy], ag_yr.at[n, dz, dy], tp_at(0, dy)).wait_recv()
        for copy in sends:
            copy.wait_send()

    def layer(n):
        def add_sum(j, total):
            return total + jnp.sum(x_buf[n, j].astype(jnp.float32), axis=-1, keepdims=True)

        count = float(devices * width)
        mean = lax.fori_loop(0, devices, add_sum, jnp.zeros((rows, 1), jnp.float32)) / count

        def add_square(j, total):
            centered = x_buf[n, j].astype(jnp.float32) - mean
            return total + jnp.sum(centered * centered, axis=-1, keepdims=True)

        var = lax.fori_loop(0, devices, add_square, jnp.zeros((rows, 1), jnp.float32)) / count
        rstd = lax.rsqrt(var + NORM_EPS)
        acc[...] = jnp.zeros_like(acc)

        def project(j, carry):
            at = pl.ds(pl.multiple_of(j * width, 128), width)
            gain = gain_ref[:, at].astype(jnp.float32)
            normed = ((x_buf[n, j].astype(jnp.float32) - mean) * rstd * gain).astype(jnp.bfloat16)
            acc[...] += jnp.dot(normed, win_ref[at, :], preferred_element_type=jnp.float32)
            return carry

        lax.fori_loop(0, devices, project, 0)
        qkv[...] = acc[...].astype(jnp.bfloat16)
        causal = lax.broadcasted_iota(jnp.int32, (rows, rows), 0) >= lax.broadcasted_iota(jnp.int32, (rows, rows), 1)
        for h in range(heads):
            q = qkv[:, h * HD:(h + 1) * HD]
            k = qkv[:, cols + h * HD:cols + (h + 1) * HD]
            v = qkv[:, 2 * cols + h * HD:2 * cols + (h + 1) * HD]
            scores = lax.dot_general(q, k, (((1,), (1,)), ((), ())), preferred_element_type=jnp.float32)
            scores = jnp.where(causal, scores * HD ** (-0.5), -jnp.inf)
            weights = jnp.exp(scores - jnp.max(scores, axis=-1, keepdims=True))
            probs = (weights / jnp.sum(weights, axis=-1, keepdims=True)).astype(jnp.bfloat16)
            ctx[:, h * HD:(h + 1) * HD] = jnp.dot(probs, v, preferred_element_type=jnp.float32).astype(jnp.bfloat16)

        def partial_for(tp):
            at = pl.ds(pl.multiple_of(tp * width, 128), width)
            return jnp.dot(ctx[...], wout_ref[:, at], preferred_element_type=jnp.float32)

        order = list(range(1, nz)) + [0]
        sends, got = [], {}
        for dz in order:
            for dy in range(1, ny):
                part[dy - 1, dz] = partial_for(tp_at(dz, dy)).astype(jnp.bfloat16)
                got[dz, dy] = copy_to(part.at[dy - 1, dz], ry_buf.at[n, dy - 1, dz],
                                      rs_ys.at[dz, dy], rs_yr.at[n, dz, dy], s, tp_at(0, dy))
                got[dz, dy].start()
        for dz in order:
            own_part[dz] = partial_for(tp_at(dz, 0))
        for dz in order:
            total = own_part[dz]
            for dy in range(1, ny):
                got[dz, dy].wait_recv()
                total = total + ry_buf[n, dy - 1, dz].astype(jnp.float32)
            if dz:
                zs_buf[dz - 1] = total.astype(jnp.bfloat16)
                sends.append(copy_to(zs_buf.at[dz - 1], rz_buf.at[n, dz - 1], rs_zs.at[dz], rs_zr.at[n, dz],
                                     s, tp_at(dz, 0)))
                sends[-1].start()
            else:
                own_part[0] = total
        total = own_part[0]
        for copy in sends:
            copy.wait_recv()
        for dz in range(1, nz):
            total = total + rz_buf[n, dz - 1].astype(jnp.float32)
        y_buf[n] = (x_buf[n, me].astype(jnp.float32) + total).astype(jnp.bfloat16)
        for copy in list(got.values()) + sends:
            copy.wait_send()

    def needed(section, n):
        tail = (n <= TICKS) | (section > 2) | (section == 0)
        live = (section + TICKS - 1 >= n) | ((section == 0) & (n == TICKS + 1))
        if sections <= TICKS + 1:
            live = live & ((section != sections - 1) | (n != TICKS - 1))
        return live & tail

    def passes(section, n):
        return needed(section, n) & (n > 0) & ((section > 0) | (n == TICKS + 1))

    def shift_copy(n):
        return copy_to(fwd_buf, x_buf.at[n, me], sh_s.at[0], sh_r.at[n], nxt, me)

    def pick(cond, a, b):
        return jnp.where(jnp.full(a.shape, cond), a, b)

    def own_rows():
        settled = pick((s < lost) | (s - TICKS + 1 > lost), y_buf[TICKS - 1], y_buf[TICKS])
        return pick(s == lost, y_buf[0], settled)

    def step(n, carry):
        @pl.when(needed(s, n))
        def _():
            @pl.when(n == 0)
            def _():
                for j in range(devices):
                    rows_j = pend_ref[0, :, j * width:(j + 1) * width]
                    x_buf[0, j] = pick(s == lost, jnp.zeros_like(rows_j), rows_j)

            @pl.when(passes(s, n))
            def _():
                shift_copy(n).wait_recv()

            @pl.when(n > 0)
            def _():
                @pl.when(jnp.logical_not(passes(s, n)))
                def _():
                    x_buf[n, me] = pool_ref[plan_ref[n - 1]]

                all_gather(n)

            layer(n)

        @pl.when(jnp.logical_not(needed(s, n)))
        def _():
            y_buf[n] = jnp.zeros((rows, width), jnp.bfloat16)

        @pl.when((n < steps - 1) & passes(nxt, n + 1))
        def _():
            fwd_buf[...] = y_buf[n]

            @pl.when((n == TICKS) & (s == sections - 1))
            def _():
                fwd_buf[...] = own_rows()

            copy = shift_copy(n + 1)
            copy.start()
            copy.wait_send()

        return carry

    lax.fori_loop(0, steps, step, 0)

    settled = pick((s - 1 < lost) | (s - TICKS > lost), y_buf[TICKS], y_buf[TICKS + 1])
    spare = pick(s - 1 == lost, y_buf[1], settled)
    spare = pick(s == 0, y_buf[TICKS + 1], spare)
    final = pick(s == lost, spare, own_rows())
    final = pick(nxt == 0, pool_ref[plan_ref[TICKS - 1]], final)
    last_buf[0] = pick(nxt == lost, jnp.zeros_like(final), final)
    last_buf[1] = spare
    out_copy = copy_to(last_buf.at[0], x_buf.at[steps, me], sh_s.at[0], sh_r.at[steps], nxt, me)
    spare_copy = copy_to(last_buf.at[1], spare_in, sh_s.at[1], sh_r.at[0], nxt, me)
    out_copy.start()
    spare_copy.start()
    out_copy.wait_recv()
    all_gather(steps)
    for j in range(devices):
        later_ref[0, :, j * width:(j + 1) * width] = x_buf[steps, j]
    spare_copy.wait_recv()
    standby_ref[0] = spare_in[...]
    out_copy.wait_send()
    spare_copy.wait_send()


def solution(mesh):
    sections, devices = mesh.shape["section"], mesh.shape["tp"]
    ny = 1
    while (2 * ny) * (2 * ny) <= devices and devices % (2 * ny) == 0:
        ny *= 2
    nz = devices // ny

    def per_device(pend, pool, plan, lost, win, wout, gain):
        rows, hidden = pend.shape[1], pend.shape[2]
        width = hidden // devices
        cols = win.shape[3]
        slots = TICKS + 3
        win = win.reshape(hidden, 3 * cols)
        vmem = pl.BlockSpec(memory_space=pltpu.VMEM)
        smem = pl.BlockSpec(memory_space=pltpu.SMEM)
        bf = functools.partial(pltpu.VMEM, dtype=jnp.bfloat16)
        dma = pltpu.SemaphoreType.DMA
        return pl.pallas_call(
            functools.partial(relay_kernel, sections, nz, ny),
            out_shape=(
                jax.ShapeDtypeStruct((1, rows, hidden), jnp.bfloat16),
                jax.ShapeDtypeStruct((1, rows, width), jnp.bfloat16),
            ),
            in_specs=[smem, smem] + [vmem] * 5,
            out_specs=(vmem, vmem),
            scratch_shapes=[
                bf((slots, devices, rows, width)),
                bf((slots, rows, width)),
                pltpu.VMEM((rows, 3 * cols), jnp.float32),
                bf((rows, 3 * cols)),
                bf((rows, cols)),
                bf((ny - 1, nz, rows, width)),
                pltpu.VMEM((nz, rows, width), jnp.float32),
                bf((slots, ny - 1, nz, rows, width)),
                bf((nz - 1, rows, width)),
                bf((slots, nz - 1, rows, width)),
                bf((rows, width)),
                bf((2, rows, width)),
                bf((rows, width)),
                dma((nz,)), dma((slots, nz)), dma((nz, ny)), dma((slots, nz, ny)),
                dma((nz,)), dma((slots, nz)), dma((nz, ny)), dma((slots, nz, ny)),
                dma((2,)), dma((slots,)),
            ],
            compiler_params=pltpu.CompilerParams(
                collective_id=0, has_side_effects=True, vmem_limit_bytes=60 * 1024 * 1024
            ),
        )(lost, plan, pend, pool, win, wout[0], gain)

    placed = (
        P("section", None, None),
        P(None, None, "tp"),
        P(),
        P(),
        P("section", None, None, "tp"),
        P("section", "tp", None),
        P("section", None),
    )
    return jax.shard_map(
        per_device,
        mesh=mesh,
        in_specs=placed,
        out_specs=(P("section", None, None), P("section", None, "tp")),
        check_vma=False,
    )
```

```python
import functools

import jax
import jax.numpy as jnp
from jax import lax
from jax.experimental import pallas as pl
from jax.experimental.pallas import tpu as pltpu
from jax.sharding import PartitionSpec as P

HD = 128
TICKS = 3
NORM_EPS = 1e-05
MESH = pl.DeviceIdType.MESH


def relay_kernel(
    sections, nz, ny,
    lost_ref, plan_ref, pend_ref, pool_ref, win_ref, wout_ref, gain_ref,
    later_ref, standby_ref,
    x_buf, y_buf, acc, qkv, ctx, part, own_part, ry_buf, zs_buf, rz_buf, fwd_buf, last_buf, spare_in,
    ag_zs, ag_zr, ag_ys, ag_yr, rs_zs, rs_zr, rs_ys, rs_yr, sh_s, sh_r,
):
    steps = TICKS + 2
    s = lax.axis_index("section")
    me = lax.axis_index("tp")
    z, y = me // ny, me % ny
    nxt, prv = (s + 1) % sections, (s + sections - 1) % sections
    lost = lost_ref[0]
    devices = nz * ny
    rows, width = x_buf.shape[2], x_buf.shape[3]
    cols = wout_ref.shape[0]
    heads = cols // HD

    def partner(at, mask):
        bit = 1
        while bit <= mask:
            if mask & bit:
                at = at + bit - 2 * bit * ((at // bit) % 2)
            bit *= 2
        return at

    def tp_at(dz, dy):
        return partner(z, dz) * ny + partner(y, dy)

    barrier = pltpu.get_barrier_semaphore()
    for dz in range(1, nz):
        pl.semaphore_signal(barrier, inc=1, device_id={"section": s, "tp": tp_at(dz, 0)}, device_id_type=MESH)
    for dy in range(1, ny):
        pl.semaphore_signal(barrier, inc=1, device_id={"section": s, "tp": tp_at(0, dy)}, device_id_type=MESH)
    pl.semaphore_signal(barrier, inc=1, device_id={"section": nxt, "tp": me}, device_id_type=MESH)
    pl.semaphore_signal(barrier, inc=1, device_id={"section": prv, "tp": me}, device_id_type=MESH)
    pl.semaphore_wait(barrier, nz + ny)

    def copy_to(src, dst, send, recv, section, tp):
        return pltpu.make_async_remote_copy(
            src_ref=src, dst_ref=dst, send_sem=send, recv_sem=recv,
            device_id={"section": section, "tp": tp}, device_id_type=MESH,
        )

    def block_copy(n, slot, send, recv, tp):
        return copy_to(x_buf.at[n, slot], x_buf.at[n, slot], send, recv, s, tp)

    def z_copy(n, dz, slot):
        return block_copy(n, slot, ag_zs.at[dz], ag_zr.at[n, dz], tp_at(dz, 0))

    def y_copy(n, dz, dy, slot):
        return block_copy(n, slot, ag_ys.at[dz, dy], ag_yr.at[n, dz, dy], tp_at(0, dy))

    def ag_start(n):
        for dz in range(1, nz):
            z_copy(n, dz, me).start()
        for dy in range(1, ny):
            y_copy(n, 0, dy, me).start()

    def ag_forward(n):
        for dz in range(1, nz):
            z_copy(n, dz, tp_at(dz, 0)).wait_recv()
            for dy in range(1, ny):
                y_copy(n, dz, dy, tp_at(dz, 0)).start()

    def ag_finish(n):
        for dz in range(nz):
            for dy in range(1, ny):
                y_copy(n, dz, dy, tp_at(dz, dy)).wait_recv()
        for dz in range(1, nz):
            z_copy(n, dz, me).wait_send()
        for dz in range(nz):
            for dy in range(1, ny):
                y_copy(n, dz, dy, tp_at(dz, 0)).wait_send()

    def layer(n):
        def add_sum(j, total):
            return total + jnp.sum(x_buf[n, j].astype(jnp.float32), axis=-1, keepdims=True)

        count = float(devices * width)
        mean = lax.fori_loop(0, devices, add_sum, jnp.zeros((rows, 1), jnp.float32)) / count

        def add_square(j, total):
            centered = x_buf[n, j].astype(jnp.float32) - mean
            return total + jnp.sum(centered * centered, axis=-1, keepdims=True)

        var = lax.fori_loop(0, devices, add_square, jnp.zeros((rows, 1), jnp.float32)) / count
        rstd = lax.rsqrt(var + NORM_EPS)
        acc[...] = jnp.zeros_like(acc)

        def project(j, carry):
            at = pl.ds(pl.multiple_of(j * width, 128), width)
            gain = gain_ref[:, at].astype(jnp.float32)
            normed = ((x_buf[n, j].astype(jnp.float32) - mean) * rstd * gain).astype(jnp.bfloat16)
            acc[...] += lax.dot_general(
                normed, win_ref[:, at], (((1,), (1,)), ((), ())), preferred_element_type=jnp.float32
            )
            return carry

        lax.fori_loop(0, devices, project, 0)
        qkv[...] = acc[...].astype(jnp.bfloat16)
        causal = lax.broadcasted_iota(jnp.int32, (rows, rows), 0) >= lax.broadcasted_iota(jnp.int32, (rows, rows), 1)
        for h in range(heads):
            q = qkv[:, h * HD:(h + 1) * HD]
            k = qkv[:, cols + h * HD:cols + (h + 1) * HD]
            v = qkv[:, 2 * cols + h * HD:2 * cols + (h + 1) * HD]
            scores = lax.dot_general(q, k, (((1,), (1,)), ((), ())), preferred_element_type=jnp.float32)
            scores = jnp.where(causal, scores * HD ** (-0.5), -jnp.inf)
            weights = jnp.exp(scores - jnp.max(scores, axis=-1, keepdims=True))
            probs = (weights / jnp.sum(weights, axis=-1, keepdims=True)).astype(jnp.bfloat16)
            ctx[:, h * HD:(h + 1) * HD] = jnp.dot(probs, v, preferred_element_type=jnp.float32).astype(jnp.bfloat16)

        def partial_for(tp):
            at = pl.ds(pl.multiple_of(tp * width, 128), width)
            return jnp.dot(ctx[...], wout_ref[:, at], preferred_element_type=jnp.float32)

        order = list(range(nz - 1, -1, -1))
        sends, got = [], {}
        for dz in order:
            for dy in range(1, ny):
                part[dy - 1, dz] = partial_for(tp_at(dz, dy)).astype(jnp.bfloat16)
                got[dz, dy] = copy_to(part.at[dy - 1, dz], ry_buf.at[n, dy - 1, dz],
                                      rs_ys.at[dz, dy], rs_yr.at[n, dz, dy], s, tp_at(0, dy))
                got[dz, dy].start()
        for dz in order:
            own_part[dz] = partial_for(tp_at(dz, 0))
        for dz in order:
            total = own_part[dz]
            for dy in range(1, ny):
                got[dz, dy].wait_recv()
                total = total + ry_buf[n, dy - 1, dz].astype(jnp.float32)
            if dz:
                zs_buf[dz - 1] = total.astype(jnp.bfloat16)
                sends.append(copy_to(zs_buf.at[dz - 1], rz_buf.at[n, dz - 1], rs_zs.at[dz], rs_zr.at[n, dz],
                                     s, tp_at(dz, 0)))
                sends[-1].start()
            else:
                own_part[0] = total
        @pl.when((s == 0) & (n < TICKS - 1))
        def _():
            ag_forward(n + 1)

        @pl.when(n == TICKS + 1)
        def _():
            ag_forward(steps)

        total = own_part[0]
        for copy in sends:
            copy.wait_recv()
        for dz in range(1, nz):
            total = total + rz_buf[n, dz - 1].astype(jnp.float32)
        y_buf[n] = (x_buf[n, me].astype(jnp.float32) + total).astype(jnp.bfloat16)
        for copy in list(got.values()) + sends:
            copy.wait_send()

    def needed(section, n):
        tail = (n <= TICKS) | (section > 2) | (section == 0)
        live = (section + TICKS - 1 >= n) | ((section == 0) & (n == TICKS + 1))
        if sections <= TICKS + 1:
            live = live & ((section != sections - 1) | (n != TICKS - 1))
        return live & tail

    def passes(section, n):
        return needed(section, n) & (n > 0) & ((section > 0) | (n == TICKS + 1))

    def shift_copy(n):
        return copy_to(fwd_buf, x_buf.at[n, me], sh_s.at[0], sh_r.at[n], nxt, me)

    def pick(cond, a, b):
        return jnp.where(jnp.full(a.shape, cond), a, b)

    def own_rows():
        settled = pick((s < lost) | (s - TICKS + 1 > lost), y_buf[TICKS - 1], y_buf[TICKS])
        return pick(s == lost, y_buf[0], settled)

    out_copy = copy_to(last_buf.at[0], x_buf.at[steps, me], sh_s.at[1], sh_r.at[steps], nxt, me)

    def step(n, carry):
        @pl.when(needed(s, n))
        def _():
            @pl.when(n == 0)
            def _():
                for j in range(devices):
                    rows_j = pend_ref[0, :, j * width:(j + 1) * width]
                    x_buf[0, j] = pick(s == lost, jnp.zeros_like(rows_j), rows_j)

            @pl.when(passes(s, n))
            def _():
                shift_copy(n).wait_recv()
                ag_start(n)
                ag_forward(n)

            @pl.when(n > 0)
            def _():
                ag_finish(n)

            @pl.when((s == 0) & (n < TICKS - 1))
            def _():
                x_buf[n + 1, me] = pool_ref[plan_ref[n]]
                ag_start(n + 1)

            @pl.when(n == TICKS + 1)
            def _():
                out_copy.wait_recv()
                ag_start(steps)

            layer(n)

        @pl.when(jnp.logical_not(needed(s, n)))
        def _():
            y_buf[n] = jnp.zeros((rows, width), jnp.bfloat16)

            @pl.when(n == TICKS + 1)
            def _():
                out_copy.wait_recv()
                ag_start(steps)
                ag_forward(steps)

        @pl.when((n < steps - 1) & passes(nxt, n + 1))
        def _():
            fwd_buf[...] = y_buf[n]

            @pl.when((n == TICKS) & (s == sections - 1))
            def _():
                fwd_buf[...] = own_rows()

            copy = shift_copy(n + 1)
            copy.start()
            copy.wait_send()

        @pl.when(n == TICKS)
        def _():
            final = pick(s == lost, y_buf[TICKS], own_rows())
            final = pick(nxt == 0, pool_ref[plan_ref[TICKS - 1]], final)
            last_buf[0] = pick(nxt == lost, jnp.zeros_like(final), final)
            out_copy.start()

        return carry

    lax.fori_loop(0, steps, step, 0)

    settled = pick((s - 1 < lost) | (s - TICKS > lost), y_buf[TICKS], y_buf[TICKS + 1])
    spare = pick(s - 1 == lost, y_buf[1], settled)
    spare = pick(s == 0, y_buf[TICKS + 1], spare)
    last_buf[1] = spare
    spare_copy = copy_to(last_buf.at[1], spare_in, sh_s.at[0], sh_r.at[0], nxt, me)
    spare_copy.start()
    ag_finish(steps)
    for j in range(devices):
        later_ref[0, :, j * width:(j + 1) * width] = x_buf[steps, j]
    spare_copy.wait_recv()
    standby_ref[0] = spare_in[...]
    out_copy.wait_send()
    spare_copy.wait_send()


def solution(mesh):
    sections, devices = mesh.shape["section"], mesh.shape["tp"]
    ny = 1
    while (2 * ny) * (2 * ny) <= devices and devices % (2 * ny) == 0:
        ny *= 2
    nz = devices // ny

    def per_device(pend, pool, plan, lost, win, wout, gain):
        rows, hidden = pend.shape[1], pend.shape[2]
        width = hidden // devices
        cols = win.shape[3]
        slots = TICKS + 3
        win = jnp.transpose(win[0], (1, 2, 0)).reshape(3 * cols, hidden)
        vmem = pl.BlockSpec(memory_space=pltpu.VMEM)
        smem = pl.BlockSpec(memory_space=pltpu.SMEM)
        bf = functools.partial(pltpu.VMEM, dtype=jnp.bfloat16)
        dma = pltpu.SemaphoreType.DMA
        return pl.pallas_call(
            functools.partial(relay_kernel, sections, nz, ny),
            out_shape=(
                jax.ShapeDtypeStruct((1, rows, hidden), jnp.bfloat16),
                jax.ShapeDtypeStruct((1, rows, width), jnp.bfloat16),
            ),
            in_specs=[smem, smem] + [vmem] * 5,
            out_specs=(vmem, vmem),
            scratch_shapes=[
                bf((slots, devices, rows, width)),
                bf((slots, rows, width)),
                pltpu.VMEM((rows, 3 * cols), jnp.float32),
                bf((rows, 3 * cols)),
                bf((rows, cols)),
                bf((ny - 1, nz, rows, width)),
                pltpu.VMEM((nz, rows, width), jnp.float32),
                bf((slots, ny - 1, nz, rows, width)),
                bf((nz - 1, rows, width)),
                bf((slots, nz - 1, rows, width)),
                bf((rows, width)),
                bf((2, rows, width)),
                bf((rows, width)),
                dma((nz,)), dma((slots, nz)), dma((nz, ny)), dma((slots, nz, ny)),
                dma((nz,)), dma((slots, nz)), dma((nz, ny)), dma((slots, nz, ny)),
                dma((2,)), dma((slots,)),
            ],
            compiler_params=pltpu.CompilerParams(
                collective_id=0, has_side_effects=True, vmem_limit_bytes=60 * 1024 * 1024
            ),
        )(lost, plan, pend, pool, win, wout[0], gain)

    placed = (
        P("section", None, None),
        P(None, None, "tp"),
        P(),
        P(),
        P("section", None, None, "tp"),
        P("section", "tp", None),
        P("section", None),
    )
    return jax.shard_map(
        per_device,
        mesh=mesh,
        in_specs=placed,
        out_specs=(P("section", None, None), P("section", None, "tp")),
        check_vma=False,
    )
```

```python
import functools

import jax
import jax.numpy as jnp
from jax import lax
from jax.experimental import pallas as pl
from jax.experimental.pallas import tpu as pltpu
from jax.sharding import PartitionSpec as P

HD = 128
TICKS = 3
NORM_EPS = 1e-05
MESH = pl.DeviceIdType.MESH


def relay_kernel(
    sections, nz, ny,
    lost_ref, plan_ref, pend_ref, pool_ref, win_hbm, wout_hbm, gain_ref,
    later_ref, standby_ref,
    win_ref, wout_ref, w_sem, x_buf, y_buf, acc, qkv, ctx, part, own_part, ry_buf, zs_buf, rz_buf, fwd_buf, last_buf, spare_in,
    ag_zs, ag_zr, ag_ys, ag_yr, rs_zs, rs_zr, rs_ys, rs_yr, sh_s, sh_r,
):
    steps = TICKS + 2
    s = lax.axis_index("section")
    me = lax.axis_index("tp")
    z, y = me // ny, me % ny
    nxt, prv = (s + 1) % sections, (s + sections - 1) % sections
    lost = lost_ref[0]
    devices = nz * ny
    rows, width = x_buf.shape[2], x_buf.shape[3]
    cols = wout_ref.shape[0]
    heads = cols // HD

    def partner(at, mask):
        bit = 1
        while bit <= mask:
            if mask & bit:
                at = at + bit - 2 * bit * ((at // bit) % 2)
            bit *= 2
        return at

    def tp_at(dz, dy):
        return partner(z, dz) * ny + partner(y, dy)

    win_copy = pltpu.make_async_copy(win_hbm, win_ref, w_sem.at[0])
    wout_copy = pltpu.make_async_copy(wout_hbm, wout_ref, w_sem.at[1])
    win_copy.start()
    wout_copy.start()
    barrier = pltpu.get_barrier_semaphore()
    for dz in range(1, nz):
        pl.semaphore_signal(barrier, inc=1, device_id={"section": s, "tp": tp_at(dz, 0)}, device_id_type=MESH)
    for dy in range(1, ny):
        pl.semaphore_signal(barrier, inc=1, device_id={"section": s, "tp": tp_at(0, dy)}, device_id_type=MESH)
    pl.semaphore_signal(barrier, inc=1, device_id={"section": nxt, "tp": me}, device_id_type=MESH)
    pl.semaphore_signal(barrier, inc=1, device_id={"section": prv, "tp": me}, device_id_type=MESH)
    pl.semaphore_wait(barrier, nz + ny)

    def copy_to(src, dst, send, recv, section, tp):
        return pltpu.make_async_remote_copy(
            src_ref=src, dst_ref=dst, send_sem=send, recv_sem=recv,
            device_id={"section": section, "tp": tp}, device_id_type=MESH,
        )

    def block_copy(n, slot, send, recv, tp):
        return copy_to(x_buf.at[n, slot], x_buf.at[n, slot], send, recv, s, tp)

    def z_copy(n, dz, slot):
        return block_copy(n, slot, ag_zs.at[dz], ag_zr.at[n, dz], tp_at(dz, 0))

    def y_copy(n, dz, dy, slot):
        return block_copy(n, slot, ag_ys.at[dz, dy], ag_yr.at[n, dz, dy], tp_at(0, dy))

    def ag_start(n):
        for dz in range(1, nz):
            z_copy(n, dz, me).start()
        for dy in range(1, ny):
            y_copy(n, 0, dy, me).start()

    def ag_forward(n):
        for dz in range(1, nz):
            z_copy(n, dz, tp_at(dz, 0)).wait_recv()
            for dy in range(1, ny):
                y_copy(n, dz, dy, tp_at(dz, 0)).start()

    def ag_finish(n):
        for dz in range(nz):
            for dy in range(1, ny):
                y_copy(n, dz, dy, tp_at(dz, dy)).wait_recv()
        for dz in range(1, nz):
            z_copy(n, dz, me).wait_send()
        for dz in range(nz):
            for dy in range(1, ny):
                y_copy(n, dz, dy, tp_at(dz, 0)).wait_send()

    def layer(n):
        def add_sum(j, total):
            return total + jnp.sum(x_buf[n, j].astype(jnp.float32), axis=-1, keepdims=True)

        count = float(devices * width)
        mean = lax.fori_loop(0, devices, add_sum, jnp.zeros((rows, 1), jnp.float32)) / count

        def add_square(j, total):
            centered = x_buf[n, j].astype(jnp.float32) - mean
            return total + jnp.sum(centered * centered, axis=-1, keepdims=True)

        var = lax.fori_loop(0, devices, add_square, jnp.zeros((rows, 1), jnp.float32)) / count
        rstd = lax.rsqrt(var + NORM_EPS)

        @pl.when(n == 0)
        def _():
            win_copy.wait()
            wout_copy.wait()

        acc[...] = jnp.zeros_like(acc)

        def project(j, carry):
            at = pl.ds(pl.multiple_of(j * width, 128), width)
            gain = gain_ref[:, at].astype(jnp.float32)
            normed = ((x_buf[n, j].astype(jnp.float32) - mean) * rstd * gain).astype(jnp.bfloat16)
            for i in range(3):
                acc[:, i * cols:(i + 1) * cols] += jnp.dot(
                    normed, win_ref[i, at, :], preferred_element_type=jnp.float32
                )
            return carry

        lax.fori_loop(0, devices, project, 0)
        qkv[...] = acc[...].astype(jnp.bfloat16)
        causal = lax.broadcasted_iota(jnp.int32, (rows, rows), 0) >= lax.broadcasted_iota(jnp.int32, (rows, rows), 1)
        for h in range(heads):
            q = qkv[:, h * HD:(h + 1) * HD]
            k = qkv[:, cols + h * HD:cols + (h + 1) * HD]
            v = qkv[:, 2 * cols + h * HD:2 * cols + (h + 1) * HD]
            scores = lax.dot_general(q, k, (((1,), (1,)), ((), ())), preferred_element_type=jnp.float32)
            scores = jnp.where(causal, scores * HD ** (-0.5), -jnp.inf)
            weights = jnp.exp(scores - jnp.max(scores, axis=-1, keepdims=True))
            probs = (weights / jnp.sum(weights, axis=-1, keepdims=True)).astype(jnp.bfloat16)
            ctx[:, h * HD:(h + 1) * HD] = jnp.dot(probs, v, preferred_element_type=jnp.float32).astype(jnp.bfloat16)

        def partial_for(tp):
            at = pl.ds(pl.multiple_of(tp * width, 128), width)
            return jnp.dot(ctx[...], wout_ref[:, at], preferred_element_type=jnp.float32)

        order = list(range(nz - 1, -1, -1))
        sends, got = [], {}
        for dz in order:
            for dy in range(1, ny):
                part[dy - 1, dz] = partial_for(tp_at(dz, dy)).astype(jnp.bfloat16)
                got[dz, dy] = copy_to(part.at[dy - 1, dz], ry_buf.at[n, dy - 1, dz],
                                      rs_ys.at[dz, dy], rs_yr.at[n, dz, dy], s, tp_at(0, dy))
                got[dz, dy].start()
        for dz in order:
            own_part[dz] = partial_for(tp_at(dz, 0))
        for dz in order:
            total = own_part[dz]
            for dy in range(1, ny):
                got[dz, dy].wait_recv()
                total = total + ry_buf[n, dy - 1, dz].astype(jnp.float32)
            if dz:
                zs_buf[dz - 1] = total.astype(jnp.bfloat16)
                sends.append(copy_to(zs_buf.at[dz - 1], rz_buf.at[n, dz - 1], rs_zs.at[dz], rs_zr.at[n, dz],
                                     s, tp_at(dz, 0)))
                sends[-1].start()
            else:
                own_part[0] = total
        @pl.when((s == 0) & (n < TICKS - 1))
        def _():
            ag_forward(n + 1)

        @pl.when(n == TICKS + 1)
        def _():
            ag_forward(steps)

        total = own_part[0]
        for copy in sends:
            copy.wait_recv()
        for dz in range(1, nz):
            total = total + rz_buf[n, dz - 1].astype(jnp.float32)
        y_buf[n] = (x_buf[n, me].astype(jnp.float32) + total).astype(jnp.bfloat16)
        for copy in list(got.values()) + sends:
            copy.wait_send()

    def needed(section, n):
        tail = (n <= TICKS) | (section > 2) | (section == 0)
        live = (section + TICKS - 1 >= n) | ((section == 0) & (n == TICKS + 1))
        if sections <= TICKS + 1:
            live = live & ((section != sections - 1) | (n != TICKS - 1))
        return live & tail

    def passes(section, n):
        return needed(section, n) & (n > 0) & ((section > 0) | (n == TICKS + 1))

    def shift_copy(n):
        return copy_to(fwd_buf, x_buf.at[n, me], sh_s.at[0], sh_r.at[n], nxt, me)

    def pick(cond, a, b):
        return jnp.where(jnp.full(a.shape, cond), a, b)

    def own_rows():
        settled = pick((s < lost) | (s - TICKS + 1 > lost), y_buf[TICKS - 1], y_buf[TICKS])
        return pick(s == lost, y_buf[0], settled)

    out_copy = copy_to(last_buf.at[0], x_buf.at[steps, me], sh_s.at[1], sh_r.at[steps], nxt, me)

    def step(n, carry):
        @pl.when(needed(s, n))
        def _():
            @pl.when(n == 0)
            def _():
                for j in range(devices):
                    rows_j = pend_ref[0, :, j * width:(j + 1) * width]
                    x_buf[0, j] = pick(s == lost, jnp.zeros_like(rows_j), rows_j)

            @pl.when(passes(s, n))
            def _():
                shift_copy(n).wait_recv()
                ag_start(n)
                ag_forward(n)

            @pl.when(n > 0)
            def _():
                ag_finish(n)

            @pl.when((s == 0) & (n < TICKS - 1))
            def _():
                x_buf[n + 1, me] = pool_ref[plan_ref[n]]
                ag_start(n + 1)

            @pl.when(n == TICKS + 1)
            def _():
                out_copy.wait_recv()
                ag_start(steps)

            layer(n)

        @pl.when(jnp.logical_not(needed(s, n)))
        def _():
            y_buf[n] = jnp.zeros((rows, width), jnp.bfloat16)

            @pl.when(n == TICKS + 1)
            def _():
                out_copy.wait_recv()
                ag_start(steps)
                ag_forward(steps)

        @pl.when((n < steps - 1) & passes(nxt, n + 1))
        def _():
            fwd_buf[...] = y_buf[n]

            @pl.when((n == TICKS) & (s == sections - 1))
            def _():
                fwd_buf[...] = own_rows()

            copy = shift_copy(n + 1)
            copy.start()
            copy.wait_send()

        @pl.when(n == TICKS)
        def _():
            final = pick(s == lost, y_buf[TICKS], own_rows())
            final = pick(nxt == 0, pool_ref[plan_ref[TICKS - 1]], final)
            last_buf[0] = pick(nxt == lost, jnp.zeros_like(final), final)
            out_copy.start()

        return carry

    lax.fori_loop(0, steps, step, 0)

    settled = pick((s - 1 < lost) | (s - TICKS > lost), y_buf[TICKS], y_buf[TICKS + 1])
    spare = pick(s - 1 == lost, y_buf[1], settled)
    spare = pick(s == 0, y_buf[TICKS + 1], spare)
    last_buf[1] = spare
    spare_copy = copy_to(last_buf.at[1], spare_in, sh_s.at[0], sh_r.at[0], nxt, me)
    spare_copy.start()
    ag_finish(steps)
    for j in range(devices):
        later_ref[0, :, j * width:(j + 1) * width] = x_buf[steps, j]
    spare_copy.wait_recv()
    standby_ref[0] = spare_in[...]
    out_copy.wait_send()
    spare_copy.wait_send()


def solution(mesh):
    sections, devices = mesh.shape["section"], mesh.shape["tp"]
    ny = 1
    while (2 * ny) * (2 * ny) <= devices and devices % (2 * ny) == 0:
        ny *= 2
    nz = devices // ny

    def per_device(pend, pool, plan, lost, win, wout, gain):
        rows, hidden = pend.shape[1], pend.shape[2]
        width = hidden // devices
        cols = win.shape[3]
        slots = TICKS + 3
        win = jnp.transpose(win[0], (1, 0, 2))
        vmem = pl.BlockSpec(memory_space=pltpu.VMEM)
        smem = pl.BlockSpec(memory_space=pltpu.SMEM)
        hbm = pl.BlockSpec(memory_space=pl.ANY)
        bf = functools.partial(pltpu.VMEM, dtype=jnp.bfloat16)
        dma = pltpu.SemaphoreType.DMA
        return pl.pallas_call(
            functools.partial(relay_kernel, sections, nz, ny),
            out_shape=(
                jax.ShapeDtypeStruct((1, rows, hidden), jnp.bfloat16),
                jax.ShapeDtypeStruct((1, rows, width), jnp.bfloat16),
            ),
            in_specs=[smem, smem, vmem, vmem, hbm, hbm, vmem],
            out_specs=(vmem, vmem),
            scratch_shapes=[
                bf((3, hidden, cols)),
                bf((cols, hidden)),
                dma((2,)),
                bf((slots, devices, rows, width)),
                bf((slots, rows, width)),
                pltpu.VMEM((rows, 3 * cols), jnp.float32),
                bf((rows, 3 * cols)),
                bf((rows, cols)),
                bf((ny - 1, nz, rows, width)),
                pltpu.VMEM((nz, rows, width), jnp.float32),
                bf((slots, ny - 1, nz, rows, width)),
                bf((nz - 1, rows, width)),
                bf((slots, nz - 1, rows, width)),
                bf((rows, width)),
                bf((2, rows, width)),
                bf((rows, width)),
                dma((nz,)), dma((slots, nz)), dma((nz, ny)), dma((slots, nz, ny)),
                dma((nz,)), dma((slots, nz)), dma((nz, ny)), dma((slots, nz, ny)),
                dma((2,)), dma((slots,)),
            ],
            compiler_params=pltpu.CompilerParams(
                collective_id=0, has_side_effects=True, vmem_limit_bytes=60 * 1024 * 1024
            ),
        )(lost, plan, pend, pool, win, wout[0], gain)

    placed = (
        P("section", None, None),
        P(None, None, "tp"),
        P(),
        P(),
        P("section", None, None, "tp"),
        P("section", "tp", None),
        P("section", None),
    )
    return jax.shard_map(
        per_device,
        mesh=mesh,
        in_specs=placed,
        out_specs=(P("section", None, None), P("section", None, "tp")),
        check_vma=False,
    )
```

```python
import functools

import jax
import jax.numpy as jnp
from jax import lax
from jax.experimental import pallas as pl
from jax.experimental.pallas import tpu as pltpu
from jax.sharding import PartitionSpec as P

HD = 128
TICKS = 3
NORM_EPS = 1e-05
MESH = pl.DeviceIdType.MESH
PIECES = 2


def relay_kernel(
    sections, nz, ny,
    lost_ref, plan_ref, pend_ref, pool_ref, win_hbm, wout_hbm, gain_ref,
    later_ref, standby_ref,
    win_ref, wout_ref, w_sem, x_buf, y_buf, acc, qkv, ctx, part, own_part, ry_buf, zs_buf, rz_buf, fwd_buf, last_buf, spare_in,
    ag_zs, ag_zr, ag_ys, ag_yr, rs_zs, rs_zr, rs_ys, rs_yr, sh_s, sh_r,
):
    steps = TICKS + 2
    s = lax.axis_index("section")
    me = lax.axis_index("tp")
    z, y = me // ny, me % ny
    nxt, prv = (s + 1) % sections, (s + sections - 1) % sections
    lost = lost_ref[0]
    devices = nz * ny
    rows, width = x_buf.shape[2], x_buf.shape[3]
    cols = wout_ref.shape[0]
    heads = cols // HD

    def partner(at, mask):
        bit = 1
        while bit <= mask:
            if mask & bit:
                at = at + bit - 2 * bit * ((at // bit) % 2)
            bit *= 2
        return at

    def tp_at(dz, dy):
        return partner(z, dz) * ny + partner(y, dy)

    win_copy = pltpu.make_async_copy(win_hbm, win_ref, w_sem.at[0])
    wout_copy = pltpu.make_async_copy(wout_hbm, wout_ref, w_sem.at[1])
    win_copy.start()
    wout_copy.start()
    barrier = pltpu.get_barrier_semaphore()
    for dz in range(1, nz):
        pl.semaphore_signal(barrier, inc=1, device_id={"section": s, "tp": tp_at(dz, 0)}, device_id_type=MESH)
    for dy in range(1, ny):
        pl.semaphore_signal(barrier, inc=1, device_id={"section": s, "tp": tp_at(0, dy)}, device_id_type=MESH)
    pl.semaphore_signal(barrier, inc=1, device_id={"section": nxt, "tp": me}, device_id_type=MESH)
    pl.semaphore_signal(barrier, inc=1, device_id={"section": prv, "tp": me}, device_id_type=MESH)
    pl.semaphore_wait(barrier, nz + ny)

    def copy_to(src, dst, send, recv, section, tp):
        return pltpu.make_async_remote_copy(
            src_ref=src, dst_ref=dst, send_sem=send, recv_sem=recv,
            device_id={"section": section, "tp": tp}, device_id_type=MESH,
        )

    def span(h):
        return pl.ds(h * (rows // PIECES), rows // PIECES)

    def block_copy(n, slot, h, send, recv, tp):
        return copy_to(x_buf.at[n, slot, span(h)], x_buf.at[n, slot, span(h)], send, recv, s, tp)

    def z_copy(n, h, dz, slot):
        return block_copy(n, slot, h, ag_zs.at[h, dz], ag_zr.at[n, h, dz], tp_at(dz, 0))

    def y_copy(n, h, dz, dy, slot):
        return block_copy(n, slot, h, ag_ys.at[h, dz, dy], ag_yr.at[n, h, dz, dy], tp_at(0, dy))

    def ag_start(n):
        for dz in range(1, nz):
            for h in range(PIECES):
                z_copy(n, h, dz, me).start()
        for dy in range(1, ny):
            for h in range(PIECES):
                y_copy(n, h, 0, dy, me).start()

    def ag_forward(n):
        for dz in range(1, nz):
            for h in range(PIECES):
                z_copy(n, h, dz, tp_at(dz, 0)).wait_recv()
                for dy in range(1, ny):
                    y_copy(n, h, dz, dy, tp_at(dz, 0)).start()

    def ag_finish(n):
        for h in range(PIECES):
            for dz in range(nz):
                for dy in range(1, ny):
                    y_copy(n, h, dz, dy, tp_at(dz, dy)).wait_recv()
            for dz in range(1, nz):
                z_copy(n, h, dz, me).wait_send()
            for dz in range(nz):
                for dy in range(1, ny):
                    y_copy(n, h, dz, dy, tp_at(dz, 0)).wait_send()

    def layer(n):
        def add_sum(j, total):
            return total + jnp.sum(x_buf[n, j].astype(jnp.float32), axis=-1, keepdims=True)

        count = float(devices * width)
        mean = lax.fori_loop(0, devices, add_sum, jnp.zeros((rows, 1), jnp.float32)) / count

        def add_square(j, total):
            centered = x_buf[n, j].astype(jnp.float32) - mean
            return total + jnp.sum(centered * centered, axis=-1, keepdims=True)

        var = lax.fori_loop(0, devices, add_square, jnp.zeros((rows, 1), jnp.float32)) / count
        rstd = lax.rsqrt(var + NORM_EPS)

        @pl.when(n == 0)
        def _():
            win_copy.wait()
            wout_copy.wait()

        acc[...] = jnp.zeros_like(acc)

        def project(j, carry):
            at = pl.ds(pl.multiple_of(j * width, 128), width)
            gain = gain_ref[:, at].astype(jnp.float32)
            normed = ((x_buf[n, j].astype(jnp.float32) - mean) * rstd * gain).astype(jnp.bfloat16)
            for i in range(3):
                acc[:, i * cols:(i + 1) * cols] += jnp.dot(
                    normed, win_ref[i, at, :], preferred_element_type=jnp.float32
                )
            return carry

        lax.fori_loop(0, devices, project, 0)
        qkv[...] = acc[...].astype(jnp.bfloat16)
        causal = lax.broadcasted_iota(jnp.int32, (rows, rows), 0) >= lax.broadcasted_iota(jnp.int32, (rows, rows), 1)
        for h in range(heads):
            q = qkv[:, h * HD:(h + 1) * HD]
            k = qkv[:, cols + h * HD:cols + (h + 1) * HD]
            v = qkv[:, 2 * cols + h * HD:2 * cols + (h + 1) * HD]
            scores = lax.dot_general(q, k, (((1,), (1,)), ((), ())), preferred_element_type=jnp.float32)
            scores = jnp.where(causal, scores * HD ** (-0.5), -jnp.inf)
            weights = jnp.exp(scores - jnp.max(scores, axis=-1, keepdims=True))
            probs = (weights / jnp.sum(weights, axis=-1, keepdims=True)).astype(jnp.bfloat16)
            ctx[:, h * HD:(h + 1) * HD] = jnp.dot(probs, v, preferred_element_type=jnp.float32).astype(jnp.bfloat16)

        def partial_for(tp):
            at = pl.ds(pl.multiple_of(tp * width, 128), width)
            return jnp.dot(ctx[...], wout_ref[:, at], preferred_element_type=jnp.float32)

        order = list(range(nz - 1, -1, -1))
        sends, got = [], {}
        for dz in order:
            for dy in range(1, ny):
                part[dy - 1, dz] = partial_for(tp_at(dz, dy)).astype(jnp.bfloat16)
                for h in range(PIECES):
                    got[dz, dy, h] = copy_to(part.at[dy - 1, dz, span(h)], ry_buf.at[n, dy - 1, dz, span(h)],
                                             rs_ys.at[h, dz, dy], rs_yr.at[n, h, dz, dy], s, tp_at(0, dy))
                    got[dz, dy, h].start()
        for dz in order:
            own_part[dz] = partial_for(tp_at(dz, 0))
        for dz in order:
            for h in range(PIECES):
                total = own_part[dz, span(h)]
                for dy in range(1, ny):
                    got[dz, dy, h].wait_recv()
                    total = total + ry_buf[n, dy - 1, dz, span(h)].astype(jnp.float32)
                if dz:
                    zs_buf[dz - 1, span(h)] = total.astype(jnp.bfloat16)
                    sends.append(copy_to(zs_buf.at[dz - 1, span(h)], rz_buf.at[n, dz - 1, span(h)],
                                         rs_zs.at[h, dz], rs_zr.at[n, h, dz], s, tp_at(dz, 0)))
                    sends[-1].start()
                else:
                    own_part[0, span(h)] = total

        @pl.when((s == 0) & (n < TICKS - 1))
        def _():
            ag_forward(n + 1)

        @pl.when(n == TICKS + 1)
        def _():
            ag_forward(steps)

        total = own_part[0]
        for copy in sends:
            copy.wait_recv()
        for dz in range(1, nz):
            total = total + rz_buf[n, dz - 1].astype(jnp.float32)
        y_buf[n] = (x_buf[n, me].astype(jnp.float32) + total).astype(jnp.bfloat16)
        for copy in list(got.values()) + sends:
            copy.wait_send()

    def needed(section, n):
        tail = (n <= TICKS) | (section > 2) | (section == 0)
        live = (section + TICKS - 1 >= n) | ((section == 0) & (n == TICKS + 1))
        if sections <= TICKS + 1:
            live = live & ((section != sections - 1) | (n != TICKS - 1))
        return live & tail

    def passes(section, n):
        return needed(section, n) & (n > 0) & ((section > 0) | (n == TICKS + 1))

    def shift_copy(n):
        return copy_to(fwd_buf, x_buf.at[n, me], sh_s.at[0], sh_r.at[n], nxt, me)

    def pick(cond, a, b):
        return jnp.where(jnp.full(a.shape, cond), a, b)

    def own_rows():
        settled = pick((s < lost) | (s - TICKS + 1 > lost), y_buf[TICKS - 1], y_buf[TICKS])
        return pick(s == lost, y_buf[0], settled)

    out_copy = copy_to(last_buf.at[0], x_buf.at[steps, me], sh_s.at[1], sh_r.at[steps], nxt, me)

    def step(n, carry):
        @pl.when(needed(s, n))
        def _():
            @pl.when(n == 0)
            def _():
                for j in range(devices):
                    rows_j = pend_ref[0, :, j * width:(j + 1) * width]
                    x_buf[0, j] = pick(s == lost, jnp.zeros_like(rows_j), rows_j)

            @pl.when(passes(s, n))
            def _():
                shift_copy(n).wait_recv()
                ag_start(n)
                ag_forward(n)

            @pl.when(n > 0)
            def _():
                ag_finish(n)

            @pl.when((s == 0) & (n < TICKS - 1))
            def _():
                x_buf[n + 1, me] = pool_ref[plan_ref[n]]
                ag_start(n + 1)

            @pl.when(n == TICKS + 1)
            def _():
                out_copy.wait_recv()
                ag_start(steps)

            layer(n)

        @pl.when(jnp.logical_not(needed(s, n)))
        def _():
            y_buf[n] = jnp.zeros((rows, width), jnp.bfloat16)

            @pl.when(n == TICKS + 1)
            def _():
                out_copy.wait_recv()
                ag_start(steps)
                ag_forward(steps)

        @pl.when((n < steps - 1) & passes(nxt, n + 1))
        def _():
            fwd_buf[...] = y_buf[n]

            @pl.when((n == TICKS) & (s == sections - 1))
            def _():
                fwd_buf[...] = own_rows()

            copy = shift_copy(n + 1)
            copy.start()
            copy.wait_send()

        @pl.when(n == TICKS)
        def _():
            final = pick(s == lost, y_buf[TICKS], own_rows())
            final = pick(nxt == 0, pool_ref[plan_ref[TICKS - 1]], final)
            last_buf[0] = pick(nxt == lost, jnp.zeros_like(final), final)
            out_copy.start()

        return carry

    lax.fori_loop(0, steps, step, 0)

    settled = pick((s - 1 < lost) | (s - TICKS > lost), y_buf[TICKS], y_buf[TICKS + 1])
    spare = pick(s - 1 == lost, y_buf[1], settled)
    spare = pick(s == 0, y_buf[TICKS + 1], spare)
    last_buf[1] = spare
    spare_copy = copy_to(last_buf.at[1], spare_in, sh_s.at[0], sh_r.at[0], nxt, me)
    spare_copy.start()
    ag_finish(steps)
    for j in range(devices):
        later_ref[0, :, j * width:(j + 1) * width] = x_buf[steps, j]
    spare_copy.wait_recv()
    standby_ref[0] = spare_in[...]
    out_copy.wait_send()
    spare_copy.wait_send()


def solution(mesh):
    sections, devices = mesh.shape["section"], mesh.shape["tp"]
    ny = 1
    while (2 * ny) * (2 * ny) <= devices and devices % (2 * ny) == 0:
        ny *= 2
    nz = devices // ny

    def per_device(pend, pool, plan, lost, win, wout, gain):
        rows, hidden = pend.shape[1], pend.shape[2]
        width = hidden // devices
        cols = win.shape[3]
        slots = TICKS + 3
        win = jnp.transpose(win[0], (1, 0, 2))
        vmem = pl.BlockSpec(memory_space=pltpu.VMEM)
        smem = pl.BlockSpec(memory_space=pltpu.SMEM)
        hbm = pl.BlockSpec(memory_space=pl.ANY)
        bf = functools.partial(pltpu.VMEM, dtype=jnp.bfloat16)
        dma = pltpu.SemaphoreType.DMA
        return pl.pallas_call(
            functools.partial(relay_kernel, sections, nz, ny),
            out_shape=(
                jax.ShapeDtypeStruct((1, rows, hidden), jnp.bfloat16),
                jax.ShapeDtypeStruct((1, rows, width), jnp.bfloat16),
            ),
            in_specs=[smem, smem, vmem, vmem, hbm, hbm, vmem],
            out_specs=(vmem, vmem),
            scratch_shapes=[
                bf((3, hidden, cols)),
                bf((cols, hidden)),
                dma((2,)),
                bf((slots, devices, rows, width)),
                bf((slots, rows, width)),
                pltpu.VMEM((rows, 3 * cols), jnp.float32),
                bf((rows, 3 * cols)),
                bf((rows, cols)),
                bf((ny - 1, nz, rows, width)),
                pltpu.VMEM((nz, rows, width), jnp.float32),
                bf((slots, ny - 1, nz, rows, width)),
                bf((nz - 1, rows, width)),
                bf((slots, nz - 1, rows, width)),
                bf((rows, width)),
                bf((2, rows, width)),
                bf((rows, width)),
                dma((PIECES, nz)), dma((slots, PIECES, nz)), dma((PIECES, nz, ny)), dma((slots, PIECES, nz, ny)),
                dma((PIECES, nz)), dma((slots, PIECES, nz)), dma((PIECES, nz, ny)), dma((slots, PIECES, nz, ny)),
                dma((2,)), dma((slots,)),
            ],
            compiler_params=pltpu.CompilerParams(
                collective_id=0, has_side_effects=True, vmem_limit_bytes=60 * 1024 * 1024
            ),
        )(lost, plan, pend, pool, win, wout[0], gain)

    placed = (
        P("section", None, None),
        P(None, None, "tp"),
        P(),
        P(),
        P("section", None, None, "tp"),
        P("section", "tp", None),
        P("section", None),
    )
    return jax.shard_map(
        per_device,
        mesh=mesh,
        in_specs=placed,
        out_specs=(P("section", None, None), P("section", None, "tp")),
        check_vma=False,
    )
```

```python
import functools

import jax
import jax.numpy as jnp
from jax import lax
from jax.experimental import pallas as pl
from jax.experimental.pallas import tpu as pltpu
from jax.sharding import PartitionSpec as P

HD = 128
TICKS = 3
NORM_EPS = 1e-05
MESH = pl.DeviceIdType.MESH
PIECES = 4


def relay_kernel(
    sections, nz, ny,
    lost_ref, plan_ref, pend_ref, pool_ref, win_hbm, wout_hbm, gain_ref,
    later_ref, standby_ref,
    win_ref, wout_ref, w_sem, x_buf, y_buf, acc, qkv, ctx, part, own_part, ry_buf, zs_buf, rz_buf, fwd_buf, last_buf, spare_in,
    ag_zs, ag_zr, ag_ys, ag_yr, rs_zs, rs_zr, rs_ys, rs_yr, sh_s, sh_r,
):
    steps = TICKS + 2
    s = lax.axis_index("section")
    me = lax.axis_index("tp")
    z, y = me // ny, me % ny
    nxt, prv = (s + 1) % sections, (s + sections - 1) % sections
    lost = lost_ref[0]
    devices = nz * ny
    rows, width = x_buf.shape[2], x_buf.shape[3]
    cols = wout_ref.shape[0]
    heads = cols // HD

    def partner(at, mask):
        bit = 1
        while bit <= mask:
            if mask & bit:
                at = at + bit - 2 * bit * ((at // bit) % 2)
            bit *= 2
        return at

    def tp_at(dz, dy):
        return partner(z, dz) * ny + partner(y, dy)

    win_copy = pltpu.make_async_copy(win_hbm, win_ref, w_sem.at[0])
    wout_copy = pltpu.make_async_copy(wout_hbm, wout_ref, w_sem.at[1])
    win_copy.start()
    wout_copy.start()
    barrier = pltpu.get_barrier_semaphore()
    for dz in range(1, nz):
        pl.semaphore_signal(barrier, inc=1, device_id={"section": s, "tp": tp_at(dz, 0)}, device_id_type=MESH)
    for dy in range(1, ny):
        pl.semaphore_signal(barrier, inc=1, device_id={"section": s, "tp": tp_at(0, dy)}, device_id_type=MESH)
    pl.semaphore_signal(barrier, inc=1, device_id={"section": nxt, "tp": me}, device_id_type=MESH)
    pl.semaphore_signal(barrier, inc=1, device_id={"section": prv, "tp": me}, device_id_type=MESH)
    pl.semaphore_wait(barrier, nz + ny)

    def copy_to(src, dst, send, recv, section, tp):
        return pltpu.make_async_remote_copy(
            src_ref=src, dst_ref=dst, send_sem=send, recv_sem=recv,
            device_id={"section": section, "tp": tp}, device_id_type=MESH,
        )

    def span(h):
        return pl.ds(h * (rows // PIECES), rows // PIECES)

    def block_copy(n, slot, h, send, recv, tp):
        return copy_to(x_buf.at[n, slot, span(h)], x_buf.at[n, slot, span(h)], send, recv, s, tp)

    def z_copy(n, h, dz, slot):
        return block_copy(n, slot, h, ag_zs.at[h, dz], ag_zr.at[n, h, dz], tp_at(dz, 0))

    def y_copy(n, h, dz, dy, slot):
        return block_copy(n, slot, h, ag_ys.at[h, dz, dy], ag_yr.at[n, h, dz, dy], tp_at(0, dy))

    def ag_start(n):
        for dz in range(1, nz):
            for h in range(PIECES):
                z_copy(n, h, dz, me).start()
        for dy in range(1, ny):
            for h in range(PIECES):
                y_copy(n, h, 0, dy, me).start()

    def ag_forward(n):
        for dz in range(1, nz):
            for h in range(PIECES):
                z_copy(n, h, dz, tp_at(dz, 0)).wait_recv()
                for dy in range(1, ny):
                    y_copy(n, h, dz, dy, tp_at(dz, 0)).start()

    def ag_finish(n):
        for h in range(PIECES):
            for dz in range(nz):
                for dy in range(1, ny):
                    y_copy(n, h, dz, dy, tp_at(dz, dy)).wait_recv()
            for dz in range(1, nz):
                z_copy(n, h, dz, me).wait_send()
            for dz in range(nz):
                for dy in range(1, ny):
                    y_copy(n, h, dz, dy, tp_at(dz, 0)).wait_send()

    def layer(n):
        def add_sum(j, total):
            return total + jnp.sum(x_buf[n, j].astype(jnp.float32), axis=-1, keepdims=True)

        count = float(devices * width)
        mean = lax.fori_loop(0, devices, add_sum, jnp.zeros((rows, 1), jnp.float32)) / count

        def add_square(j, total):
            centered = x_buf[n, j].astype(jnp.float32) - mean
            return total + jnp.sum(centered * centered, axis=-1, keepdims=True)

        var = lax.fori_loop(0, devices, add_square, jnp.zeros((rows, 1), jnp.float32)) / count
        rstd = lax.rsqrt(var + NORM_EPS)

        @pl.when(n == 0)
        def _():
            win_copy.wait()
            wout_copy.wait()

        acc[...] = jnp.zeros_like(acc)

        def project(j, carry):
            at = pl.ds(pl.multiple_of(j * width, 128), width)
            gain = gain_ref[:, at].astype(jnp.float32)
            normed = ((x_buf[n, j].astype(jnp.float32) - mean) * rstd * gain).astype(jnp.bfloat16)
            for i in range(3):
                acc[:, i * cols:(i + 1) * cols] += jnp.dot(
                    normed, win_ref[i, at, :], preferred_element_type=jnp.float32
                )
            return carry

        lax.fori_loop(0, devices, project, 0)
        qkv[...] = acc[...].astype(jnp.bfloat16)
        causal = lax.broadcasted_iota(jnp.int32, (rows, rows), 0) >= lax.broadcasted_iota(jnp.int32, (rows, rows), 1)
        for h in range(heads):
            q = qkv[:, h * HD:(h + 1) * HD]
            k = qkv[:, cols + h * HD:cols + (h + 1) * HD]
            v = qkv[:, 2 * cols + h * HD:2 * cols + (h + 1) * HD]
            scores = lax.dot_general(q, k, (((1,), (1,)), ((), ())), preferred_element_type=jnp.float32)
            scores = jnp.where(causal, scores * HD ** (-0.5), -jnp.inf)
            weights = jnp.exp(scores - jnp.max(scores, axis=-1, keepdims=True))
            probs = (weights / jnp.sum(weights, axis=-1, keepdims=True)).astype(jnp.bfloat16)
            ctx[:, h * HD:(h + 1) * HD] = jnp.dot(probs, v, preferred_element_type=jnp.float32).astype(jnp.bfloat16)

        def partial_for(tp):
            at = pl.ds(pl.multiple_of(tp * width, 128), width)
            return jnp.dot(ctx[...], wout_ref[:, at], preferred_element_type=jnp.float32)

        order = list(range(nz - 1, -1, -1))
        sends, got = [], {}
        for dz in order:
            for dy in range(1, ny):
                part[dy - 1, dz] = partial_for(tp_at(dz, dy)).astype(jnp.bfloat16)
                for h in range(PIECES):
                    got[dz, dy, h] = copy_to(part.at[dy - 1, dz, span(h)], ry_buf.at[n, dy - 1, dz, span(h)],
                                             rs_ys.at[h, dz, dy], rs_yr.at[n, h, dz, dy], s, tp_at(0, dy))
                    got[dz, dy, h].start()
        for dz in order:
            own_part[dz] = partial_for(tp_at(dz, 0))
        for dz in order:
            for h in range(PIECES):
                total = own_part[dz, span(h)]
                for dy in range(1, ny):
                    got[dz, dy, h].wait_recv()
                    total = total + ry_buf[n, dy - 1, dz, span(h)].astype(jnp.float32)
                if dz:
                    zs_buf[dz - 1, span(h)] = total.astype(jnp.bfloat16)
                    sends.append(copy_to(zs_buf.at[dz - 1, span(h)], rz_buf.at[n, dz - 1, span(h)],
                                         rs_zs.at[h, dz], rs_zr.at[n, h, dz], s, tp_at(dz, 0)))
                    sends[-1].start()
                else:
                    own_part[0, span(h)] = total

        @pl.when((s == 0) & (n < TICKS - 1))
        def _():
            ag_forward(n + 1)

        @pl.when(n == TICKS + 1)
        def _():
            ag_forward(steps)

        total = own_part[0]
        for copy in sends:
            copy.wait_recv()
        for dz in range(1, nz):
            total = total + rz_buf[n, dz - 1].astype(jnp.float32)
        y_buf[n] = (x_buf[n, me].astype(jnp.float32) + total).astype(jnp.bfloat16)
        for copy in list(got.values()) + sends:
            copy.wait_send()

    def needed(section, n):
        tail = (n <= TICKS) | (section > 2) | (section == 0)
        live = (section + TICKS - 1 >= n) | ((section == 0) & (n == TICKS + 1))
        if sections <= TICKS + 1:
            live = live & ((section != sections - 1) | (n != TICKS - 1))
        return live & tail

    def passes(section, n):
        return needed(section, n) & (n > 0) & ((section > 0) | (n == TICKS + 1))

    def shift_copy(n):
        return copy_to(fwd_buf, x_buf.at[n, me], sh_s.at[0], sh_r.at[n], nxt, me)

    def pick(cond, a, b):
        return jnp.where(jnp.full(a.shape, cond), a, b)

    def own_rows():
        settled = pick((s < lost) | (s - TICKS + 1 > lost), y_buf[TICKS - 1], y_buf[TICKS])
        return pick(s == lost, y_buf[0], settled)

    out_copy = copy_to(last_buf.at[0], x_buf.at[steps, me], sh_s.at[1], sh_r.at[steps], nxt, me)

    def step(n, carry):
        @pl.when(needed(s, n))
        def _():
            @pl.when(n == 0)
            def _():
                for j in range(devices):
                    rows_j = pend_ref[0, :, j * width:(j + 1) * width]
                    x_buf[0, j] = pick(s == lost, jnp.zeros_like(rows_j), rows_j)

            @pl.when(passes(s, n))
            def _():
                shift_copy(n).wait_recv()
                ag_start(n)
                ag_forward(n)

            @pl.when(n > 0)
            def _():
                ag_finish(n)

            @pl.when((s == 0) & (n < TICKS - 1))
            def _():
                x_buf[n + 1, me] = pool_ref[plan_ref[n]]
                ag_start(n + 1)

            @pl.when(n == TICKS + 1)
            def _():
                out_copy.wait_recv()
                ag_start(steps)

            layer(n)

        @pl.when(jnp.logical_not(needed(s, n)))
        def _():
            y_buf[n] = jnp.zeros((rows, width), jnp.bfloat16)

            @pl.when(n == TICKS + 1)
            def _():
                out_copy.wait_recv()
                ag_start(steps)
                ag_forward(steps)

        @pl.when((n < steps - 1) & passes(nxt, n + 1))
        def _():
            fwd_buf[...] = y_buf[n]

            @pl.when((n == TICKS) & (s == sections - 1))
            def _():
                fwd_buf[...] = own_rows()

            copy = shift_copy(n + 1)
            copy.start()
            copy.wait_send()

        @pl.when(n == TICKS)
        def _():
            final = pick(s == lost, y_buf[TICKS], own_rows())
            final = pick(nxt == 0, pool_ref[plan_ref[TICKS - 1]], final)
            last_buf[0] = pick(nxt == lost, jnp.zeros_like(final), final)
            out_copy.start()

        return carry

    lax.fori_loop(0, steps, step, 0)

    settled = pick((s - 1 < lost) | (s - TICKS > lost), y_buf[TICKS], y_buf[TICKS + 1])
    spare = pick(s - 1 == lost, y_buf[1], settled)
    spare = pick(s == 0, y_buf[TICKS + 1], spare)
    last_buf[1] = spare
    spare_copy = copy_to(last_buf.at[1], spare_in, sh_s.at[0], sh_r.at[0], nxt, me)
    spare_copy.start()
    ag_finish(steps)
    for j in range(devices):
        later_ref[0, :, j * width:(j + 1) * width] = x_buf[steps, j]
    spare_copy.wait_recv()
    standby_ref[0] = spare_in[...]
    out_copy.wait_send()
    spare_copy.wait_send()


def solution(mesh):
    sections, devices = mesh.shape["section"], mesh.shape["tp"]
    ny = 1
    while (2 * ny) * (2 * ny) <= devices and devices % (2 * ny) == 0:
        ny *= 2
    nz = devices // ny

    def per_device(pend, pool, plan, lost, win, wout, gain):
        rows, hidden = pend.shape[1], pend.shape[2]
        width = hidden // devices
        cols = win.shape[3]
        slots = TICKS + 3
        win = jnp.transpose(win[0], (1, 0, 2))
        vmem = pl.BlockSpec(memory_space=pltpu.VMEM)
        smem = pl.BlockSpec(memory_space=pltpu.SMEM)
        hbm = pl.BlockSpec(memory_space=pl.ANY)
        bf = functools.partial(pltpu.VMEM, dtype=jnp.bfloat16)
        dma = pltpu.SemaphoreType.DMA
        return pl.pallas_call(
            functools.partial(relay_kernel, sections, nz, ny),
            out_shape=(
                jax.ShapeDtypeStruct((1, rows, hidden), jnp.bfloat16),
                jax.ShapeDtypeStruct((1, rows, width), jnp.bfloat16),
            ),
            in_specs=[smem, smem, vmem, vmem, hbm, hbm, vmem],
            out_specs=(vmem, vmem),
            scratch_shapes=[
                bf((3, hidden, cols)),
                bf((cols, hidden)),
                dma((2,)),
                bf((slots, devices, rows, width)),
                bf((slots, rows, width)),
                pltpu.VMEM((rows, 3 * cols), jnp.float32),
                bf((rows, 3 * cols)),
                bf((rows, cols)),
                bf((ny - 1, nz, rows, width)),
                pltpu.VMEM((nz, rows, width), jnp.float32),
                bf((slots, ny - 1, nz, rows, width)),
                bf((nz - 1, rows, width)),
                bf((slots, nz - 1, rows, width)),
                bf((rows, width)),
                bf((2, rows, width)),
                bf((rows, width)),
                dma((PIECES, nz)), dma((slots, PIECES, nz)), dma((PIECES, nz, ny)), dma((slots, PIECES, nz, ny)),
                dma((PIECES, nz)), dma((slots, PIECES, nz)), dma((PIECES, nz, ny)), dma((slots, PIECES, nz, ny)),
                dma((2,)), dma((slots,)),
            ],
            compiler_params=pltpu.CompilerParams(
                collective_id=0, has_side_effects=True, vmem_limit_bytes=60 * 1024 * 1024
            ),
        )(lost, plan, pend, pool, win, wout[0], gain)

    placed = (
        P("section", None, None),
        P(None, None, "tp"),
        P(),
        P(),
        P("section", None, None, "tp"),
        P("section", "tp", None),
        P("section", None),
    )
    return jax.shard_map(
        per_device,
        mesh=mesh,
        in_specs=placed,
        out_specs=(P("section", None, None), P("section", None, "tp")),
        check_vma=False,
    )
```
